32 devices in a mesh: ty: 4 (over y, x), tx: 8 (over z, core).
Axes of the slice: x: 2, y: 2, z: 4, core: 2. Of those that a mesh axis runs over, the one named last changes fastest.
Arguments:
- surface_levels: float32 [512, 16384], P('ty', 'tx'), may hold values from -6 to 6
- bearing_index: int32 [4], replicated, may hold values from 0 to 15
- stencil_displacements: int32 [4], replicated, may hold values from -4 to 4
- camera_altitude_class: int32 [4], replicated, may hold values from 0 to 3
Outputs:
- margin: float32 [4, 512, 16384], P(None, 'ty', 'tx')
The draws below stay inside these ranges and needn't reach their ends.
Inputs may be any that keep to these rules, and one draw needn't show every extreme that they name: `bearing_index`: azimuth indices.
All inputs are finite; a program needn't handle non-finite values.
Results may differ from the reference program's by a relative error of at most 0.00002.
Values sent between devices are 32-bit elements; how exact they have to be, the bound alone decides.
A program may use at most 192 MiB of HBM per device.

```python
import math
import jax
import jax.numpy as jnp
from jax import lax

AZIMUTHS = 4
STENCIL_REACH = 4
GRID_LENGTH = 512
GRID_WIDTH = 16384


def place_ends(result, stream_key, least, top_value):
    spot = [jax.random.randint(jax.random.fold_in(stream_key, axis), (), 0, length) for axis, length in enumerate(result.shape)]
    widest = result.shape.index(max(result.shape))
    beside = spot[:widest] + [(spot[widest] + 1) % result.shape[widest]] + spot[widest + 1:]
    return result.at[tuple(spot)].set(least).at[tuple(beside)].set(top_value)


def block_scale(stream_key, shape, shards, least, top_value):
    level = 1.0
    for axis_at, shards_of in shards:
        draws = jax.random.uniform(jax.random.fold_in(jax.random.fold_in(stream_key, 6), axis_at), (shards_of,), jnp.float32, least / len(shards), top_value / len(shards))
        level = level * jnp.repeat(jnp.exp(draws), shape[axis_at] // shards_of).reshape((-1,) + (1,) * (len(shape) - 1 - axis_at))
    return level


def scatter_about(own_key, dims, width, bound, pieces=(), held_as=jnp.bfloat16):
    result = width * jax.random.normal(own_key, dims, jnp.float32)
    if pieces:
        result = result * block_scale(own_key, dims, pieces, -0.22, 0.18)
    return jnp.clip(result, -bound, bound).astype(held_as)


def setup_inputs(seed: int = 0) -> dict:
    key_list = jax.random.split(jax.random.key(seed), 5)
    surface_levels = scatter_about(key_list[0], (GRID_LENGTH, GRID_WIDTH), 1.0, 6.0, ((0, 4), (1, 8)), jnp.float32)
    bearing_index = place_ends(jax.random.randint(key_list[1], (AZIMUTHS,), 0, 16), jax.random.fold_in(key_list[1], 1), 0, 15).astype(jnp.int32)
    stencil_displacements = place_ends(jax.random.randint(key_list[2], (AZIMUTHS,), -STENCIL_REACH, STENCIL_REACH + 1), jax.random.fold_in(key_list[2], 1), -STENCIL_REACH, STENCIL_REACH).astype(jnp.int32)
    camera_altitude_class = place_ends(jax.random.randint(key_list[3], (AZIMUTHS,), 0, 4), jax.random.fold_in(key_list[3], 1), 0, 3).astype(jnp.int32)
    return {"surface_levels": surface_levels, "bearing_index": bearing_index, "stencil_displacements": stencil_displacements, "camera_altitude_class": camera_altitude_class}


def view_tables(bearing_index, camera_altitude_class, easting_span):
    angle_idx = bearing_index.astype(jnp.float32)
    frac = (((bearing_index * 5) % 16).astype(jnp.float32) + 0.5) / 16.0
    theta = (angle_idx - 7.5) * (math.pi / 32.0)
    stride = 1.0 / jnp.cos(theta)
    slope = (1.0 + camera_altitude_class.astype(jnp.float32)) / (4.0 * easting_span)
    cube = frac * frac * frac
    square = frac * frac
    weights = jnp.stack([(-cube + 2.0 * square - frac) / 2.0, (3.0 * cube - 5.0 * square + 2.0) / 2.0, (-3.0 * cube + 4.0 * square + frac) / 2.0, (cube - square) / 2.0], axis=1)
    return weights, stride * slope


def reference(surface_levels, bearing_index, stencil_displacements, camera_altitude_class):
    northing_extent, easting_span = surface_levels.shape
    weights, rise = view_tables(bearing_index, camera_altitude_class, easting_span)
    border_lines = STENCIL_REACH + 2
    bordered_surface = jnp.pad(surface_levels, ((border_lines, border_lines), (0, 0)))
    columns = jnp.arange(easting_span).astype(jnp.float32)
    outputs = []
    for which in range(AZIMUTHS):
        strips = jnp.zeros((northing_extent, easting_span), jnp.float32)
        for tap_index in range(4):
            start = (stencil_displacements[which] + tap_index + STENCIL_REACH + 1).astype(jnp.int32)
            strips = strips + weights[which, tap_index] * lax.dynamic_slice_in_dim(bordered_surface, start, northing_extent, 0)
        lifted = strips + rise[which] * columns[None, :]
        running = lax.cummax(lifted, axis=1)
        lowest = jnp.full((northing_extent, 1), -jnp.inf, jnp.float32)
        horizon = jnp.concatenate([lowest, running[:, :-1]], axis=1)
        outputs.append(jnp.maximum(horizon - lifted, 0.0))
    return jnp.stack(outputs, axis=0)
```

```python
import functools
import math

import jax
import jax.numpy as jnp
from jax import lax
from jax.experimental import pallas as pl
from jax.experimental.pallas import tpu as pltpu
from jax.sharding import PartitionSpec as P

AZIMUTHS = 4
STENCIL_REACH = 4
LANES = 128
SUB = 8
MESH = pl.DeviceIdType.MESH


def view_rows(bearing, camera, easting_span):
    shape = (SUB, LANES)
    a = jnp.full(shape, bearing, jnp.int32).astype(jnp.float32)
    b = jnp.full(shape, lax.rem(bearing * 5, 16), jnp.int32).astype(jnp.float32)
    cam = jnp.full(shape, camera, jnp.int32).astype(jnp.float32)
    frac = (b + 0.5) / 16.0
    theta = (a - 7.5) * (math.pi / 32.0)
    stride = 1.0 / jnp.cos(theta)
    slope = (1.0 + cam) / (4.0 * easting_span)
    cube = frac * frac * frac
    square = frac * frac
    weights = (
        (-cube + 2.0 * square - frac) / 2.0,
        (3.0 * cube - 5.0 * square + 2.0) / 2.0,
        (-3.0 * cube + 4.0 * square + frac) / 2.0,
        (cube - square) / 2.0,
    )
    return weights, stride * slope


def exchange_kernel(
    bearing_ref, shift_ref, camera_ref, surface_hbm,
    lifted_ref, running_ref, before_ref,
    surf, above, below, edge, peaks, edge_peaks, message, inbox,
    load_sem, up_send, up_recv, down_send, down_recv, peak_send, peak_recv,
):
    rows, cols = surface_hbm.shape
    chunks, tiles = cols // LANES, rows // SUB
    ny, nx = lax.axis_size("ty"), lax.axis_size("tx")
    ty, tx = lax.axis_index("ty"), lax.axis_index("tx")
    barrier = pltpu.get_barrier_semaphore()

    def load(c):
        return pltpu.make_async_copy(
            surface_hbm.at[:, pl.ds(c * LANES, LANES)], surf.at[c], load_sem.at[c]
        )

    for c in range(chunks):
        load(c).start()

    @pl.when(ty > 0)
    def _():
        pl.semaphore_signal(barrier, 1, device_id={"ty": ty - 1}, device_id_type=MESH)

    @pl.when(ty < ny - 1)
    def _():
        pl.semaphore_signal(barrier, 1, device_id={"ty": ty + 1}, device_id_type=MESH)

    for i in range(nx - 1):

        @pl.when(i < tx)
        def _():
            pl.semaphore_signal(barrier, 1, device_id={"tx": i}, device_id_type=MESH)

    weights, rise = [], []
    for k in range(AZIMUTHS):
        w, s = view_rows(bearing_ref[k], camera_ref[k], cols * nx)
        weights.append(w)
        rise.append(s)
    lane = lax.broadcasted_iota(jnp.int32, (SUB, LANES), 1)
    first = (tx * cols + lane).astype(jnp.float32)

    for c in range(chunks):
        load(c).wait()
    sends = jnp.where(ty > 0, 1, 0) + jnp.where(ty < ny - 1, 1, 0) + (nx - 1 - tx)
    pl.semaphore_wait(barrier, sends)

    def to_above():
        return pltpu.make_async_remote_copy(
            surf.at[:, pl.ds(0, SUB), :], below, up_send, up_recv,
            device_id={"ty": ty - 1}, device_id_type=MESH,
        )

    def to_below():
        return pltpu.make_async_remote_copy(
            surf.at[:, pl.ds(rows - SUB, SUB), :], above, down_send, down_recv,
            device_id={"ty": ty + 1}, device_id_type=MESH,
        )

    @pl.when(ty < ny - 1)
    def _():
        to_below().start()

    @pl.when(ty > 0)
    def _():
        to_above().start()

    def stencil(read, row):
        top = [None] * AZIMUTHS
        for c in range(chunks):
            col = first + float(c * LANES)
            for k in range(AZIMUTHS):
                acc = weights[k][0] * read(c, k, 0)
                for j in range(1, 4):
                    acc = acc + weights[k][j] * read(c, k, j)
                acc = acc + rise[k] * col
                lifted_ref[k, c, pl.ds(row, SUB), :] = acc
                top[k] = acc if c == 0 else jnp.maximum(top[k], acc)
        return top

    def inner(t, _):
        row = pl.multiple_of(t * SUB, SUB)
        top = stencil(
            lambda c, k, j: surf[c, pl.ds(row + shift_ref[k] + (j - 1), SUB), :], row
        )
        for k in range(AZIMUTHS):
            peaks[k, pl.ds(row, SUB), :] = top[k]
        return 0

    lowest = jnp.full((SUB, LANES), -jnp.inf, jnp.float32)
    for k in range(AZIMUTHS):
        peaks[k, pl.ds(0, SUB), :] = lowest
        peaks[k, pl.ds(rows - SUB, SUB), :] = lowest
    lax.fori_loop(1, tiles - 1, inner, 0)
    for k in range(AZIMUTHS):
        message[pl.ds(k, 1), :] = jnp.max(peaks[k].T, axis=0, keepdims=True)
    message[pl.ds(AZIMUTHS, SUB - AZIMUTHS), :] = jnp.full(
        (SUB - AZIMUTHS, rows), -jnp.inf, jnp.float32
    )
    before_ref[...] = jnp.full(before_ref.shape, -jnp.inf, jnp.float32)

    @pl.when(ty == 0)
    def _():
        above[...] = jnp.zeros(above.shape, jnp.float32)

    @pl.when(ty == ny - 1)
    def _():
        below[...] = jnp.zeros(below.shape, jnp.float32)

    @pl.when(ty < ny - 1)
    def _():
        to_below().wait_send()
        to_above().wait_recv()

    @pl.when(ty > 0)
    def _():
        to_above().wait_send()
        to_below().wait_recv()

    for c in range(chunks):
        edge[0, c, pl.ds(0, SUB), :] = above[c]
        edge[0, c, pl.ds(SUB, 2 * SUB), :] = surf[c, pl.ds(0, 2 * SUB), :]
        edge[1, c, pl.ds(0, 2 * SUB), :] = surf[c, pl.ds(rows - 2 * SUB, 2 * SUB), :]
        edge[1, c, pl.ds(2 * SUB, SUB), :] = below[c]
    for e in range(2):
        top = stencil(
            lambda c, k, j: edge[e, c, pl.ds(SUB + shift_ref[k] + (j - 1), SUB), :],
            e * (rows - SUB),
        )
        for k in range(AZIMUTHS):
            edge_peaks[pl.ds((2 * k + e) * SUB, SUB), :] = top[k]
    for q in range(2 * AZIMUTHS, LANES // SUB):
        edge_peaks[pl.ds(q * SUB, SUB), :] = lowest
    message[pl.ds(AZIMUTHS, 1), pl.ds(0, LANES)] = jnp.max(
        edge_peaks[...].T, axis=0, keepdims=True
    )

    def to_right(i):
        return pltpu.make_async_remote_copy(
            message, inbox.at[tx], peak_send.at[i], peak_recv.at[tx],
            device_id={"tx": i}, device_id_type=MESH,
        )

    def from_left(i):
        return pltpu.make_async_remote_copy(
            message, inbox.at[i], peak_send.at[i], peak_recv.at[i],
            device_id={"tx": i}, device_id_type=MESH,
        )

    for i in reversed(range(1, nx)):

        @pl.when(i > tx)
        def _():
            to_right(i).start()

    def scan(q, _):
        k = q // tiles
        row = pl.multiple_of((q % tiles) * SUB, SUB)
        carry = None
        for c in range(chunks):
            x = lifted_ref[k, c, pl.ds(row, SUB), :]
            step = 1
            while step < LANES:
                rolled = pltpu.roll(x, step, axis=1)
                x = jnp.maximum(x, jnp.where(lane >= step, rolled, x))
                step *= 2
            last = jnp.broadcast_to(x[:, LANES - 1 :], (SUB, LANES))
            running_ref[k, c, pl.ds(row, SUB), :] = x if c == 0 else jnp.maximum(x, carry)
            carry = last if c == 0 else jnp.maximum(carry, last)
        return 0

    lax.fori_loop(0, AZIMUTHS * tiles, scan, 0)

    for i in range(nx):

        @pl.when(i > tx)
        def _():
            to_right(i).wait_send()

        @pl.when(i < tx)
        def _():
            from_left(i).wait_recv()
            before_ref[...] = jnp.maximum(before_ref[...], inbox[i])


def margin_kernel(lifted_ref, running_ref, before_ref, out_hbm, staged, wide, edge_wide, sem):
    _, chunks, rows, _ = lifted_ref.shape
    tiles = rows // SUB

    def put(k):
        return pltpu.make_async_copy(staged.at[k], out_hbm.at[k], sem.at[k])

    edges = before_ref[pl.ds(AZIMUTHS, 1), pl.ds(0, LANES)]
    edge_wide[...] = jnp.broadcast_to(edges, (LANES, LANES)).T
    for k in range(AZIMUTHS):
        wide[...] = jnp.broadcast_to(before_ref[pl.ds(k, 1), :], (LANES, rows)).T
        wide[pl.ds(0, SUB), :] = edge_wide[pl.ds(2 * k * SUB, SUB), :]
        wide[pl.ds(rows - SUB, SUB), :] = edge_wide[pl.ds((2 * k + 1) * SUB, SUB), :]

        def one(t, _):
            row = pl.multiple_of(t * SUB, SUB)
            bound = wide[pl.ds(row, SUB), :]
            for c in range(chunks):
                high = jnp.maximum(running_ref[k, c, pl.ds(row, SUB), :], bound)
                staged[k, pl.ds(row, SUB), pl.ds(c * LANES, LANES)] = (
                    high - lifted_ref[k, c, pl.ds(row, SUB), :]
                )
            return 0

        lax.fori_loop(0, tiles, one, 0)
        put(k).start()
    for k in range(AZIMUTHS):
        put(k).wait()


def on_device(surface_levels, bearing_index, stencil_displacements, camera_altitude_class):
    rows, cols = surface_levels.shape
    chunks = cols // LANES
    nx = lax.axis_size("tx")
    f32 = jnp.float32
    dma = pltpu.SemaphoreType.DMA
    smem = pl.BlockSpec(memory_space=pltpu.SMEM)
    vmem = pl.BlockSpec(memory_space=pltpu.VMEM)
    hbm = pl.BlockSpec(memory_space=pltpu.HBM)
    block = (AZIMUTHS, chunks, rows, LANES)
    lifted, running, before = pl.pallas_call(
        exchange_kernel,
        out_shape=(pltpu.VMEM(block, f32), pltpu.VMEM(block, f32), pltpu.VMEM((SUB, rows), f32)),
        in_specs=[smem, smem, smem, hbm],
        out_specs=(vmem, vmem, vmem),
        scratch_shapes=[
            pltpu.VMEM((chunks, rows, LANES), f32),
            pltpu.VMEM((chunks, SUB, LANES), f32),
            pltpu.VMEM((chunks, SUB, LANES), f32),
            pltpu.VMEM((2, chunks, 3 * SUB, LANES), f32),
            pltpu.VMEM((AZIMUTHS, rows, LANES), f32),
            pltpu.VMEM((LANES, LANES), f32),
            pltpu.VMEM((SUB, rows), f32),
            pltpu.VMEM((nx, SUB, rows), f32),
            dma((chunks,)),
            dma, dma, dma, dma,
            dma((nx,)),
            dma((nx,)),
        ],
        compiler_params=pltpu.CompilerParams(
            collective_id=0, has_side_effects=True, vmem_limit_bytes=24 * 2**20
        ),
        name="exchange",
    )(bearing_index, stencil_displacements, camera_altitude_class, surface_levels)
    return pl.pallas_call(
        margin_kernel,
        out_shape=jax.ShapeDtypeStruct((AZIMUTHS, rows, cols), f32),
        in_specs=[vmem, vmem, vmem],
        out_specs=hbm,
        scratch_shapes=[
            pltpu.VMEM((AZIMUTHS, rows, cols), f32),
            pltpu.VMEM((rows, LANES), f32),
            pltpu.VMEM((LANES, LANES), f32),
            dma((AZIMUTHS,)),
        ],
        compiler_params=pltpu.CompilerParams(vmem_limit_bytes=24 * 2**20),
        name="margin",
    )(lifted, running, before)


def solution(mesh):
    return jax.shard_map(
        on_device,
        mesh=mesh,
        in_specs=(P("ty", "tx"), P(), P(), P()),
        out_specs=P(None, "ty", "tx"),
        check_vma=False,
    )
```

```python
import functools
import math

import jax
import jax.numpy as jnp
from jax import lax
from jax.experimental import pallas as pl
from jax.experimental.pallas import tpu as pltpu
from jax.sharding import PartitionSpec as P

AZIMUTHS = 4
STENCIL_REACH = 4
LANES = 128
SUB = 8
MESH = pl.DeviceIdType.MESH


def view_rows(bearing, camera, easting_span):
    shape = (SUB, LANES)
    a = jnp.full(shape, bearing, jnp.int32).astype(jnp.float32)
    b = jnp.full(shape, lax.rem(bearing * 5, 16), jnp.int32).astype(jnp.float32)
    cam = jnp.full(shape, camera, jnp.int32).astype(jnp.float32)
    frac = (b + 0.5) / 16.0
    theta = (a - 7.5) * (math.pi / 32.0)
    stride = 1.0 / jnp.cos(theta)
    slope = (1.0 + cam) / (4.0 * easting_span)
    cube = frac * frac * frac
    square = frac * frac
    weights = (
        (-cube + 2.0 * square - frac) / 2.0,
        (3.0 * cube - 5.0 * square + 2.0) / 2.0,
        (-3.0 * cube + 4.0 * square + frac) / 2.0,
        (cube - square) / 2.0,
    )
    return weights, stride * slope


def exchange_kernel(
    bearing_ref, shift_ref, camera_ref, surface_hbm,
    lifted_ref, running_ref, before_ref,
    surf, above, below, edge, peaks, edge_peaks, message, inbox, turned, edge_lift,
    load_sem, up_send, up_recv, down_send, down_recv, peak_send, peak_recv,
):
    rows, cols = surface_hbm.shape
    chunks, tiles = cols // LANES, rows // SUB
    ny, nx = lax.axis_size("ty"), lax.axis_size("tx")
    ty, tx = lax.axis_index("ty"), lax.axis_index("tx")
    barrier = pltpu.get_barrier_semaphore()

    def load(c):
        return pltpu.make_async_copy(
            surface_hbm.at[:, pl.ds(c * LANES, LANES)], surf.at[c], load_sem.at[c]
        )

    for c in range(chunks):
        load(c).start()

    @pl.when(ty > 0)
    def _():
        pl.semaphore_signal(barrier, 1, device_id={"ty": ty - 1}, device_id_type=MESH)

    @pl.when(ty < ny - 1)
    def _():
        pl.semaphore_signal(barrier, 1, device_id={"ty": ty + 1}, device_id_type=MESH)

    for i in range(nx - 1):

        @pl.when(i < tx)
        def _():
            pl.semaphore_signal(barrier, 1, device_id={"tx": i}, device_id_type=MESH)

    weights, rise = [], []
    for k in range(AZIMUTHS):
        w, s = view_rows(bearing_ref[k], camera_ref[k], cols * nx)
        weights.append(w)
        rise.append(s)
    lane = lax.broadcasted_iota(jnp.int32, (SUB, LANES), 1)
    first = (tx * cols + lane).astype(jnp.float32)

    for c in range(chunks):
        load(c).wait()
    sends = jnp.where(ty > 0, 1, 0) + jnp.where(ty < ny - 1, 1, 0) + (nx - 1 - tx)
    pl.semaphore_wait(barrier, sends)

    def to_above():
        return pltpu.make_async_remote_copy(
            surf.at[:, pl.ds(0, SUB), :], below, up_send, up_recv,
            device_id={"ty": ty - 1}, device_id_type=MESH,
        )

    def to_below():
        return pltpu.make_async_remote_copy(
            surf.at[:, pl.ds(rows - SUB, SUB), :], above, down_send, down_recv,
            device_id={"ty": ty + 1}, device_id_type=MESH,
        )

    @pl.when(ty < ny - 1)
    def _():
        to_below().start()

    @pl.when(ty > 0)
    def _():
        to_above().start()

    def stencil(read, row, e=None):
        top = [None] * AZIMUTHS
        for c in range(chunks):
            col = first + float(c * LANES)
            for k in range(AZIMUTHS):
                acc = weights[k][0] * read(c, k, 0)
                for j in range(1, 4):
                    acc = acc + weights[k][j] * read(c, k, j)
                acc = acc + rise[k] * col
                lifted_ref[k, c, pl.ds(row, SUB), :] = acc
                if e is not None:
                    edge_lift[c, pl.ds((2 * k + e) * SUB, SUB), :] = acc
                top[k] = acc if c == 0 else jnp.maximum(top[k], acc)
        return top

    def inner(t, _):
        row = pl.multiple_of(t * SUB, SUB)
        top = stencil(
            lambda c, k, j: surf[c, pl.ds(row + shift_ref[k] + (j - 1), SUB), :], row
        )
        for k in range(AZIMUTHS):
            peaks[k, pl.ds(row, SUB), :] = top[k]
        return 0

    lowest = jnp.full((SUB, LANES), -jnp.inf, jnp.float32)
    for k in range(AZIMUTHS):
        peaks[k, pl.ds(0, SUB), :] = lowest
        peaks[k, pl.ds(rows - SUB, SUB), :] = lowest
    lax.fori_loop(1, tiles - 1, inner, 0)
    for k in range(AZIMUTHS):
        message[pl.ds(k, 1), :] = jnp.max(peaks[k].T, axis=0, keepdims=True)
    message[pl.ds(AZIMUTHS, SUB - AZIMUTHS), :] = jnp.full(
        (SUB - AZIMUTHS, rows), -jnp.inf, jnp.float32
    )
    before_ref[...] = jnp.full(before_ref.shape, -jnp.inf, jnp.float32)

    group = LANES // SUB
    sub = lax.broadcasted_iota(jnp.int32, (SUB, LANES), 0)
    span = max(n for n in (1, 2, 4) if chunks % n == 0)
    pair = 2 if chunks % 2 == 0 else 1

    def scan_blocks(blocks, carries):
        for slot, (load_block, _, _) in enumerate(blocks):
            turned[slot] = load_block().T
        for slot, (_, _, chain) in enumerate(blocks):
            run = []
            for v in range(group):
                x = turned[slot, pl.ds(v, SUB, stride=group), :]
                run.append(x if v == 0 else jnp.maximum(run[-1], x))
            total = run[-1]
            for step in (1, 2, 4):
                moved = pltpu.roll(total, step, axis=0)
                total = jnp.maximum(total, jnp.where(sub >= step, moved, total))
            carry = carries[chain]
            shifted = jnp.where(sub >= 1, pltpu.roll(total, 1, axis=0), carry)
            offset = jnp.maximum(shifted, carry)
            last = jnp.broadcast_to(total[SUB - 1 :, :], (SUB, LANES))
            carries[chain] = jnp.maximum(carry, last)
            for v in range(group):
                turned[slot, pl.ds(v, SUB, stride=group), :] = jnp.maximum(run[v], offset)
        for slot, (_, store_block, _) in enumerate(blocks):
            store_block(turned[slot].T)
        return carries

    def inner_scan(q, carries):
        def load(k, c):
            return lambda: lifted_ref[k, q * pair + c]

        def store(k, c):
            def put(x):
                running_ref[k, q * pair + c] = x

            return put

        blocks = [
            (load(k, c), store(k, c), k) for c in range(pair) for k in range(AZIMUTHS)
        ]
        return tuple(scan_blocks(blocks, list(carries)))

    lax.fori_loop(0, chunks // pair, inner_scan, (lowest,) * AZIMUTHS)
    for c in range(chunks):
        edge_lift[c, pl.ds(2 * AZIMUTHS * SUB, LANES - 2 * AZIMUTHS * SUB), :] = jnp.zeros(
            (LANES - 2 * AZIMUTHS * SUB, LANES), jnp.float32
        )

    @pl.when(ty == 0)
    def _():
        above[...] = jnp.zeros(above.shape, jnp.float32)

    @pl.when(ty == ny - 1)
    def _():
        below[...] = jnp.zeros(below.shape, jnp.float32)

    @pl.when(ty < ny - 1)
    def _():
        to_below().wait_send()
        to_above().wait_recv()

    @pl.when(ty > 0)
    def _():
        to_above().wait_send()
        to_below().wait_recv()

    for c in range(chunks):
        edge[0, c, pl.ds(0, SUB), :] = above[c]
        edge[0, c, pl.ds(SUB, 2 * SUB), :] = surf[c, pl.ds(0, 2 * SUB), :]
        edge[1, c, pl.ds(0, 2 * SUB), :] = surf[c, pl.ds(rows - 2 * SUB, 2 * SUB), :]
        edge[1, c, pl.ds(2 * SUB, SUB), :] = below[c]
    for e in range(2):
        top = stencil(
            lambda c, k, j: edge[e, c, pl.ds(SUB + shift_ref[k] + (j - 1), SUB), :],
            e * (rows - SUB),
            e,
        )
        for k in range(AZIMUTHS):
            edge_peaks[pl.ds((2 * k + e) * SUB, SUB), :] = top[k]
    for q in range(2 * AZIMUTHS, LANES // SUB):
        edge_peaks[pl.ds(q * SUB, SUB), :] = lowest
    message[pl.ds(AZIMUTHS, 1), pl.ds(0, LANES)] = jnp.max(
        edge_peaks[...].T, axis=0, keepdims=True
    )

    def to_right(i):
        return pltpu.make_async_remote_copy(
            message, inbox.at[tx], peak_send.at[i], peak_recv.at[tx],
            device_id={"tx": i}, device_id_type=MESH,
        )

    def from_left(i):
        return pltpu.make_async_remote_copy(
            message, inbox.at[i], peak_send.at[i], peak_recv.at[i],
            device_id={"tx": i}, device_id_type=MESH,
        )

    for i in reversed(range(1, nx)):

        @pl.when(i > tx)
        def _():
            to_right(i).start()

    def edge_scan(q, carry):
        def load(c):
            return lambda: edge_lift[q * span + c]

        def store(c):
            def put(x):
                for k in range(AZIMUTHS):
                    at = 2 * k * SUB
                    running_ref[k, q * span + c, pl.ds(0, SUB), :] = x[at : at + SUB]
                    running_ref[k, q * span + c, pl.ds(rows - SUB, SUB), :] = (
                        x[at + SUB : at + 2 * SUB]
                    )

            return put

        blocks = [(load(c), store(c), 0) for c in range(span)]
        return tuple(scan_blocks(blocks, [carry[0]]))

    lax.fori_loop(0, chunks // span, edge_scan, (lowest,))

    for i in range(nx):

        @pl.when(i > tx)
        def _():
            to_right(i).wait_send()

        @pl.when(i < tx)
        def _():
            from_left(i).wait_recv()
            before_ref[...] = jnp.maximum(before_ref[...], inbox[i])


def margin_kernel(lifted_ref, running_ref, before_ref, out_hbm, staged, wide, edge_wide, sem):
    _, chunks, rows, _ = lifted_ref.shape
    tiles = rows // SUB

    def put(k):
        return pltpu.make_async_copy(staged.at[k], out_hbm.at[k], sem.at[k])

    edges = before_ref[pl.ds(AZIMUTHS, 1), pl.ds(0, LANES)]
    edge_wide[...] = jnp.broadcast_to(edges, (LANES, LANES)).T
    for k in range(AZIMUTHS):
        wide[...] = jnp.broadcast_to(before_ref[pl.ds(k, 1), :], (LANES, rows)).T
        wide[pl.ds(0, SUB), :] = edge_wide[pl.ds(2 * k * SUB, SUB), :]
        wide[pl.ds(rows - SUB, SUB), :] = edge_wide[pl.ds((2 * k + 1) * SUB, SUB), :]

        def one(t, _):
            row = pl.multiple_of(t * SUB, SUB)
            bound = wide[pl.ds(row, SUB), :]
            for c in range(chunks):
                high = jnp.maximum(running_ref[k, c, pl.ds(row, SUB), :], bound)
                staged[k, pl.ds(row, SUB), pl.ds(c * LANES, LANES)] = (
                    high - lifted_ref[k, c, pl.ds(row, SUB), :]
                )
            return 0

        lax.fori_loop(0, tiles, one, 0)
        put(k).start()
    for k in range(AZIMUTHS):
        put(k).wait()


def on_device(surface_levels, bearing_index, stencil_displacements, camera_altitude_class):
    rows, cols = surface_levels.shape
    chunks = cols // LANES
    nx = lax.axis_size("tx")
    f32 = jnp.float32
    dma = pltpu.SemaphoreType.DMA
    smem = pl.BlockSpec(memory_space=pltpu.SMEM)
    vmem = pl.BlockSpec(memory_space=pltpu.VMEM)
    hbm = pl.BlockSpec(memory_space=pltpu.HBM)
    block = (AZIMUTHS, chunks, rows, LANES)
    lifted, running, before = pl.pallas_call(
        exchange_kernel,
        out_shape=(pltpu.VMEM(block, f32), pltpu.VMEM(block, f32), pltpu.VMEM((SUB, rows), f32)),
        in_specs=[smem, smem, smem, hbm],
        out_specs=(vmem, vmem, vmem),
        scratch_shapes=[
            pltpu.VMEM((chunks, rows, LANES), f32),
            pltpu.VMEM((chunks, SUB, LANES), f32),
            pltpu.VMEM((chunks, SUB, LANES), f32),
            pltpu.VMEM((2, chunks, 3 * SUB, LANES), f32),
            pltpu.VMEM((AZIMUTHS, rows, LANES), f32),
            pltpu.VMEM((LANES, LANES), f32),
            pltpu.VMEM((SUB, rows), f32),
            pltpu.VMEM((nx, SUB, rows), f32),
            pltpu.VMEM((2 * AZIMUTHS, LANES, LANES), f32),
            pltpu.VMEM((chunks, LANES, LANES), f32),
            dma((chunks,)),
            dma, dma, dma, dma,
            dma((nx,)),
            dma((nx,)),
        ],
        compiler_params=pltpu.CompilerParams(
            collective_id=0, has_side_effects=True, vmem_limit_bytes=56 * 2**20 - 2**17
        ),
        name="exchange",
    )(bearing_index, stencil_displacements, camera_altitude_class, surface_levels)
    return pl.pallas_call(
        margin_kernel,
        out_shape=jax.ShapeDtypeStruct((AZIMUTHS, rows, cols), f32),
        in_specs=[vmem, vmem, vmem],
        out_specs=hbm,
        scratch_shapes=[
            pltpu.VMEM((AZIMUTHS, rows, cols), f32),
            pltpu.VMEM((rows, LANES), f32),
            pltpu.VMEM((LANES, LANES), f32),
            dma((AZIMUTHS,)),
        ],
        compiler_params=pltpu.CompilerParams(vmem_limit_bytes=24 * 2**20),
        name="margin",
    )(lifted, running, before)


def solution(mesh):
    return jax.shard_map(
        on_device,
        mesh=mesh,
        in_specs=(P("ty", "tx"), P(), P(), P()),
        out_specs=P(None, "ty", "tx"),
        check_vma=False,
    )
```

```python
import functools
import math

import jax
import jax.numpy as jnp
from jax import lax
from jax.experimental import pallas as pl
from jax.experimental.pallas import tpu as pltpu
from jax.sharding import PartitionSpec as P

AZIMUTHS = 4
STENCIL_REACH = 4
LANES = 128
SUB = 8
MESH = pl.DeviceIdType.MESH


def view_rows(bearing, camera, easting_span):
    shape = (SUB, LANES)
    a = jnp.full(shape, bearing, jnp.int32).astype(jnp.float32)
    b = jnp.full(shape, lax.rem(bearing * 5, 16), jnp.int32).astype(jnp.float32)
    cam = jnp.full(shape, camera, jnp.int32).astype(jnp.float32)
    frac = (b + 0.5) / 16.0
    theta = (a - 7.5) * (math.pi / 32.0)
    stride = 1.0 / jnp.cos(theta)
    slope = (1.0 + cam) / (4.0 * easting_span)
    cube = frac * frac * frac
    square = frac * frac
    weights = (
        (-cube + 2.0 * square - frac) / 2.0,
        (3.0 * cube - 5.0 * square + 2.0) / 2.0,
        (-3.0 * cube + 4.0 * square + frac) / 2.0,
        (cube - square) / 2.0,
    )
    return weights, stride * slope


def exchange_kernel(
    bearing_ref, shift_ref, camera_ref, surface_hbm,
    lifted_ref, running_ref, before_ref,
    surf, above, below, edge, peaks, edge_peaks, message, inbox, turned, edge_lift,
    load_sem, up_send, up_recv, down_send, down_recv, peak_send, peak_recv,
):
    rows, cols = surface_hbm.shape
    chunks, tiles = cols // LANES, rows // SUB
    ny, nx = lax.axis_size("ty"), lax.axis_size("tx")
    ty, tx = lax.axis_index("ty"), lax.axis_index("tx")
    barrier = pltpu.get_barrier_semaphore()

    def load(c):
        return pltpu.make_async_copy(
            surface_hbm.at[:, pl.ds(c * LANES, LANES)], surf.at[c], load_sem.at[c]
        )

    for c in range(chunks):
        load(c).start()

    @pl.when(ty > 0)
    def _():
        pl.semaphore_signal(barrier, 1, device_id={"ty": ty - 1}, device_id_type=MESH)

    @pl.when(ty < ny - 1)
    def _():
        pl.semaphore_signal(barrier, 1, device_id={"ty": ty + 1}, device_id_type=MESH)

    for i in range(nx - 1):

        @pl.when(i < tx)
        def _():
            pl.semaphore_signal(barrier, 1, device_id={"tx": i}, device_id_type=MESH)

    weights, rise = [], []
    for k in range(AZIMUTHS):
        w, s = view_rows(bearing_ref[k], camera_ref[k], cols * nx)
        weights.append(w)
        rise.append(s)
    lane = lax.broadcasted_iota(jnp.int32, (SUB, LANES), 1)
    first = (tx * cols + lane).astype(jnp.float32)

    for c in range(chunks):
        load(c).wait()
    def to_above():
        return pltpu.make_async_remote_copy(
            surf.at[:, pl.ds(0, SUB), :], below, up_send, up_recv,
            device_id={"ty": ty - 1}, device_id_type=MESH,
        )

    def to_below():
        return pltpu.make_async_remote_copy(
            surf.at[:, pl.ds(rows - SUB, SUB), :], above, down_send, down_recv,
            device_id={"ty": ty + 1}, device_id_type=MESH,
        )

    def stencil(read, row, e=None):
        top = [None] * AZIMUTHS
        for c in range(chunks):
            col = first + float(c * LANES)
            for k in range(AZIMUTHS):
                acc = weights[k][0] * read(c, k, 0)
                for j in range(1, 4):
                    acc = acc + weights[k][j] * read(c, k, j)
                acc = acc + rise[k] * col
                lifted_ref[k, c, pl.ds(row, SUB), :] = acc
                if e is not None:
                    edge_lift[c, pl.ds((2 * k + e) * SUB, SUB), :] = acc
                top[k] = acc if c == 0 else jnp.maximum(top[k], acc)
        return top

    def inner(t, _):
        row = pl.multiple_of(t * SUB, SUB)
        top = stencil(
            lambda c, k, j: surf[c, pl.ds(row + shift_ref[k] + (j - 1), SUB), :], row
        )
        for k in range(AZIMUTHS):
            peaks[k, pl.ds(row, SUB), :] = top[k]
        return 0

    lowest = jnp.full((SUB, LANES), -jnp.inf, jnp.float32)
    for k in range(AZIMUTHS):
        peaks[k, pl.ds(0, SUB), :] = lowest
        peaks[k, pl.ds(rows - SUB, SUB), :] = lowest
    early = 1 + (tiles - 2) * (nx - tx) // nx
    lax.fori_loop(1, early, inner, 0)
    sends = jnp.where(ty > 0, 1, 0) + jnp.where(ty < ny - 1, 1, 0) + (nx - 1 - tx)
    pl.semaphore_wait(barrier, sends)

    @pl.when(ty < ny - 1)
    def _():
        to_below().start()

    @pl.when(ty > 0)
    def _():
        to_above().start()

    lax.fori_loop(early, tiles - 1, inner, 0)
    for k in range(AZIMUTHS):
        message[pl.ds(k, 1), :] = jnp.max(peaks[k].T, axis=0, keepdims=True)
    message[pl.ds(AZIMUTHS, SUB - AZIMUTHS), :] = jnp.full(
        (SUB - AZIMUTHS, rows), -jnp.inf, jnp.float32
    )
    before_ref[...] = jnp.full(before_ref.shape, -jnp.inf, jnp.float32)

    group = LANES // SUB
    sub = lax.broadcasted_iota(jnp.int32, (SUB, LANES), 0)
    span = max(n for n in (1, 2, 4) if chunks % n == 0)
    pair = 2 if chunks % 2 == 0 else 1

    def scan_blocks(blocks, carries):
        for slot, (load_block, _, _) in enumerate(blocks):
            turned[slot] = load_block().T
        for slot, (_, _, chain) in enumerate(blocks):
            run = []
            for v in range(group):
                x = turned[slot, pl.ds(v, SUB, stride=group), :]
                run.append(x if v == 0 else jnp.maximum(run[-1], x))
            total = run[-1]
            for step in (1, 2, 4):
                moved = pltpu.roll(total, step, axis=0)
                total = jnp.maximum(total, jnp.where(sub >= step, moved, total))
            carry = carries[chain]
            shifted = jnp.where(sub >= 1, pltpu.roll(total, 1, axis=0), carry)
            offset = jnp.maximum(shifted, carry)
            last = jnp.broadcast_to(total[SUB - 1 :, :], (SUB, LANES))
            carries[chain] = jnp.maximum(carry, last)
            for v in range(group):
                turned[slot, pl.ds(v, SUB, stride=group), :] = jnp.maximum(run[v], offset)
        for slot, (_, store_block, _) in enumerate(blocks):
            store_block(turned[slot].T)
        return carries

    def inner_scan(q, carries):
        def load(k, c):
            return lambda: lifted_ref[k, q * pair + c]

        def store(k, c):
            def put(x):
                running_ref[k, q * pair + c] = x

            return put

        blocks = [
            (load(k, c), store(k, c), k) for c in range(pair) for k in range(AZIMUTHS)
        ]
        return tuple(scan_blocks(blocks, list(carries)))

    lax.fori_loop(0, chunks // pair, inner_scan, (lowest,) * AZIMUTHS)
    for c in range(chunks):
        edge_lift[c, pl.ds(2 * AZIMUTHS * SUB, LANES - 2 * AZIMUTHS * SUB), :] = jnp.zeros(
            (LANES - 2 * AZIMUTHS * SUB, LANES), jnp.float32
        )

    @pl.when(ty == 0)
    def _():
        above[...] = jnp.zeros(above.shape, jnp.float32)

    @pl.when(ty == ny - 1)
    def _():
        below[...] = jnp.zeros(below.shape, jnp.float32)

    @pl.when(ty < ny - 1)
    def _():
        to_below().wait_send()
        to_above().wait_recv()

    @pl.when(ty > 0)
    def _():
        to_above().wait_send()
        to_below().wait_recv()

    for c in range(chunks):
        edge[0, c, pl.ds(0, SUB), :] = above[c]
        edge[0, c, pl.ds(SUB, 2 * SUB), :] = surf[c, pl.ds(0, 2 * SUB), :]
        edge[1, c, pl.ds(0, 2 * SUB), :] = surf[c, pl.ds(rows - 2 * SUB, 2 * SUB), :]
        edge[1, c, pl.ds(2 * SUB, SUB), :] = below[c]
    for e in range(2):
        top = stencil(
            lambda c, k, j: edge[e, c, pl.ds(SUB + shift_ref[k] + (j - 1), SUB), :],
            e * (rows - SUB),
            e,
        )
        for k in range(AZIMUTHS):
            edge_peaks[pl.ds((2 * k + e) * SUB, SUB), :] = top[k]
    for q in range(2 * AZIMUTHS, LANES // SUB):
        edge_peaks[pl.ds(q * SUB, SUB), :] = lowest
    message[pl.ds(AZIMUTHS, 1), pl.ds(0, LANES)] = jnp.max(
        edge_peaks[...].T, axis=0, keepdims=True
    )

    def to_right(i):
        return pltpu.make_async_remote_copy(
            message, inbox.at[tx], peak_send.at[i], peak_recv.at[tx],
            device_id={"tx": i}, device_id_type=MESH,
        )

    def from_left(i):
        return pltpu.make_async_remote_copy(
            message, inbox.at[i], peak_send.at[i], peak_recv.at[i],
            device_id={"tx": i}, device_id_type=MESH,
        )

    for i in reversed(range(1, nx)):

        @pl.when(i > tx)
        def _():
            to_right(i).start()

    def edge_scan(q, carry):
        def load(c):
            return lambda: edge_lift[q * span + c]

        def store(c):
            def put(x):
                for k in range(AZIMUTHS):
                    at = 2 * k * SUB
                    running_ref[k, q * span + c, pl.ds(0, SUB), :] = x[at : at + SUB]
                    running_ref[k, q * span + c, pl.ds(rows - SUB, SUB), :] = (
                        x[at + SUB : at + 2 * SUB]
                    )

            return put

        blocks = [(load(c), store(c), 0) for c in range(span)]
        return tuple(scan_blocks(blocks, [carry[0]]))

    lax.fori_loop(0, chunks // span, edge_scan, (lowest,))

    for i in range(nx):

        @pl.when(i > tx)
        def _():
            to_right(i).wait_send()

        @pl.when(i < tx)
        def _():
            from_left(i).wait_recv()
            before_ref[...] = jnp.maximum(before_ref[...], inbox[i])


def margin_kernel(lifted_ref, running_ref, before_ref, out_hbm, staged, wide, edge_wide, sem):
    _, chunks, rows, _ = lifted_ref.shape
    tiles = rows // SUB

    def put(k):
        return pltpu.make_async_copy(staged.at[k], out_hbm.at[k], sem.at[k])

    edges = before_ref[pl.ds(AZIMUTHS, 1), pl.ds(0, LANES)]
    edge_wide[...] = jnp.broadcast_to(edges, (LANES, LANES)).T
    for k in range(AZIMUTHS):
        wide[...] = jnp.broadcast_to(before_ref[pl.ds(k, 1), :], (LANES, rows)).T
        wide[pl.ds(0, SUB), :] = edge_wide[pl.ds(2 * k * SUB, SUB), :]
        wide[pl.ds(rows - SUB, SUB), :] = edge_wide[pl.ds((2 * k + 1) * SUB, SUB), :]

        def one(t, _):
            row = pl.multiple_of(t * SUB, SUB)
            bound = wide[pl.ds(row, SUB), :]
            for c in range(chunks):
                high = jnp.maximum(running_ref[k, c, pl.ds(row, SUB), :], bound)
                staged[k, pl.ds(row, SUB), pl.ds(c * LANES, LANES)] = (
                    high - lifted_ref[k, c, pl.ds(row, SUB), :]
                )
            return 0

        lax.fori_loop(0, tiles, one, 0)
        put(k).start()
    for k in range(AZIMUTHS):
        put(k).wait()


def on_device(surface_levels, bearing_index, stencil_displacements, camera_altitude_class):
    rows, cols = surface_levels.shape
    chunks = cols // LANES
    nx = lax.axis_size("tx")
    f32 = jnp.float32
    dma = pltpu.SemaphoreType.DMA
    smem = pl.BlockSpec(memory_space=pltpu.SMEM)
    vmem = pl.BlockSpec(memory_space=pltpu.VMEM)
    hbm = pl.BlockSpec(memory_space=pltpu.HBM)
    block = (AZIMUTHS, chunks, rows, LANES)
    lifted, running, before = pl.pallas_call(
        exchange_kernel,
        out_shape=(pltpu.VMEM(block, f32), pltpu.VMEM(block, f32), pltpu.VMEM((SUB, rows), f32)),
        in_specs=[smem, smem, smem, hbm],
        out_specs=(vmem, vmem, vmem),
        scratch_shapes=[
            pltpu.VMEM((chunks, rows, LANES), f32),
            pltpu.VMEM((chunks, SUB, LANES), f32),
            pltpu.VMEM((chunks, SUB, LANES), f32),
            pltpu.VMEM((2, chunks, 3 * SUB, LANES), f32),
            pltpu.VMEM((AZIMUTHS, rows, LANES), f32),
            pltpu.VMEM((LANES, LANES), f32),
            pltpu.VMEM((SUB, rows), f32),
            pltpu.VMEM((nx, SUB, rows), f32),
            pltpu.VMEM((2 * AZIMUTHS, LANES, LANES), f32),
            pltpu.VMEM((chunks, LANES, LANES), f32),
            dma((chunks,)),
            dma, dma, dma, dma,
            dma((nx,)),
            dma((nx,)),
        ],
        compiler_params=pltpu.CompilerParams(
            collective_id=0, has_side_effects=True, vmem_limit_bytes=56 * 2**20 - 2**17
        ),
        name="exchange",
    )(bearing_index, stencil_displacements, camera_altitude_class, surface_levels)
    return pl.pallas_call(
        margin_kernel,
        out_shape=jax.ShapeDtypeStruct((AZIMUTHS, rows, cols), f32),
        in_specs=[vmem, vmem, vmem],
        out_specs=hbm,
        scratch_shapes=[
            pltpu.VMEM((AZIMUTHS, rows, cols), f32),
            pltpu.VMEM((rows, LANES), f32),
            pltpu.VMEM((LANES, LANES), f32),
            dma((AZIMUTHS,)),
        ],
        compiler_params=pltpu.CompilerParams(vmem_limit_bytes=24 * 2**20),
        name="margin",
    )(lifted, running, before)


def solution(mesh):
    return jax.shard_map(
        on_device,
        mesh=mesh,
        in_specs=(P("ty", "tx"), P(), P(), P()),
        out_specs=P(None, "ty", "tx"),
        check_vma=False,
    )
```
